32 devices in a mesh: tile: 8 (over z, y), lev: 4 (over x, core).
Axes of the slice: x: 2, y: 2, z: 4, core: 2. Of those that a mesh axis runs over, the one named last changes fastest.
Arguments:
- ensemble: bfloat16 [80, 32, 4096], P(None, 'lev', 'tile')
- pair_first: int32 [32768], P('tile'), may hold values from 0 to 511
- pair_second: int32 [32768], P('tile'), may hold values from 0 to 1023
- pair_bin: int32 [32768], P('tile'), may hold values from 0 to 63, as said below
Outputs:
- level_variance: float32 [32], P('lev')
- bin_corr: float32 [32, 64], P('lev', 'tile')
- bin_avg: float32 [64], P('tile')
The draws below stay inside these ranges and needn't reach their ends.
Inputs may be any that keep to these rules, and one draw needn't show every extreme that they name: `pair_bin`: some bins receive no pair; which ones changes with the draw.
All inputs are finite; a program needn't handle non-finite values.
Results may differ from the reference program's by a relative error of at most 0.0017.
Values may be sent and summed in bfloat16 or wider, within the bound.
A program may use at most 64 MiB of HBM per device.

```python
import jax
import jax.numpy as jnp
from jax import lax

MEMBERS = 80
LEVELS = 32
COL_DEV = 512
PAIRS_DEV = 4096
COLS = 4096
NPAIRS = 32768
NBINS = 64


def draw_ensemble(key, part):
    keys = jax.random.split(jax.random.fold_in(key, 7), 5)
    level_scale = jnp.exp(jax.random.uniform(keys[0], (1, LEVELS, 1), jnp.float32, -1.2, 1.2))
    factor = jax.random.normal(keys[1], (MEMBERS, LEVELS, 2), jnp.float32)
    loading = jax.random.uniform(keys[2], (2, LEVELS, COLS), jnp.float32, -1.2, 1.2)
    offset = 2.0 * jax.random.normal(keys[4], (1, LEVELS, COLS), jnp.float32)
    noise = jax.random.normal(keys[3], (MEMBERS, LEVELS, COLS), jnp.float32)
    colscale = jnp.ones((1, 1, COLS), jnp.float32)
    shared = factor[:, :, 0:1] * loading[0][None] + factor[:, :, 1:2] * loading[1][None]
    return (level_scale * colscale * (shared + noise) + offset).astype(jnp.bfloat16)


def draw_pair_bin(key, part):
    keys = jax.random.split(jax.random.fold_in(key, 11), 3)
    skipped = NBINS // 8
    inner = (1 + jax.random.permutation(keys[0], NBINS - 2)).astype(jnp.int32)
    kept = inner[skipped:]
    half = kept.shape[0] // 2
    ends = jnp.array([0, NBINS - 1], dtype=jnp.int32)
    table = jnp.concatenate([kept[:half], ends, kept[half:]])
    allowed = table.shape[0]
    first = jax.random.randint(keys[1], (NPAIRS,), 0, allowed, dtype=jnp.int32)
    second = jax.random.randint(keys[2], (NPAIRS,), 0, allowed, dtype=jnp.int32)
    rank = jnp.minimum(first, second)
    return jnp.take(table, rank).astype(jnp.int32)


def place_ends(values, stream_key, smallest, largest):
    spot = [jax.random.randint(jax.random.fold_in(stream_key, axis), (), 0, length) for axis, length in enumerate(values.shape)]
    longest = values.shape.index(max(values.shape))
    beside = spot[:longest] + [(spot[longest] + 1) % values.shape[longest]] + spot[longest + 1:]
    return values.at[tuple(spot)].set(smallest).at[tuple(beside)].set(largest)


def setup_inputs(seed: int = 0) -> dict:
    streams_of = jax.random.split(jax.random.key(seed), 5)
    ensemble = draw_ensemble(jax.random.fold_in(streams_of[4], 71), 0)
    pair_first = place_ends(jax.random.randint(streams_of[1], (NPAIRS,), 0, COL_DEV), jax.random.fold_in(streams_of[1], 1), 0, COL_DEV - 1).astype(jnp.int32)
    pair_second = place_ends(jax.random.randint(streams_of[2], (NPAIRS,), 0, 2 * COL_DEV), jax.random.fold_in(streams_of[2], 1), 0, (2 * COL_DEV) - 1).astype(jnp.int32)
    pair_bin = draw_pair_bin(jax.random.fold_in(streams_of[4], 71), 0)
    return {"ensemble": ensemble, "pair_first": pair_first, "pair_second": pair_second, "pair_bin": pair_bin}


def perturb(block):
    values = block.astype(jnp.float32)
    return (values - lax.optimization_barrier(jnp.mean(values, axis=0, keepdims=True))).astype(jnp.bfloat16)

def reference(ensemble, pair_first, pair_second, pair_bin):
    ntile = COLS // COL_DEV

    def tile_terms(tile):
        own = lax.dynamic_slice_in_dim(ensemble, (tile * COL_DEV).astype(jnp.int32), COL_DEV, 2)
        nxt = lax.dynamic_slice_in_dim(ensemble, ((tile + 1) % ntile * COL_DEV).astype(jnp.int32), COL_DEV, 2)
        pert_own = perturb(own).astype(jnp.float32)
        pert_ext = jnp.concatenate([pert_own, perturb(nxt).astype(jnp.float32)], axis=2)
        spread = jnp.sqrt(lax.optimization_barrier(jnp.sum(pert_ext * pert_ext, axis=0)) / (MEMBERS - 1) + 1e-06)
        squares = lax.optimization_barrier(jnp.sum(pert_own * pert_own, axis=(0, 2)))
        start = (tile * PAIRS_DEV).astype(jnp.int32)
        first = lax.dynamic_slice_in_dim(pair_first, start, PAIRS_DEV, 0)
        second = lax.dynamic_slice_in_dim(pair_second, start, PAIRS_DEV, 0)
        bins = lax.dynamic_slice_in_dim(pair_bin, start, PAIRS_DEV, 0)
        left = jnp.take(pert_ext, first, axis=2)
        right = jnp.take(pert_ext, second, axis=2)
        cov = lax.optimization_barrier(jnp.sum(left * right, axis=0)) / (MEMBERS - 1)
        corr = cov / (jnp.take(spread, first, axis=1) * jnp.take(spread, second, axis=1))
        onehot = (bins[:, None] == jnp.arange(NBINS, dtype=jnp.int32)[None, :]).astype(jnp.float32)
        sums = jnp.dot(corr, onehot, precision=lax.Precision.HIGHEST)
        return (sums, lax.optimization_barrier(jnp.sum(onehot, axis=0)), squares)
    sums, counts, squares = lax.map(tile_terms, jnp.arange(ntile, dtype=jnp.int32))
    bin_sum = lax.optimization_barrier(jnp.sum(sums, axis=0))
    bin_count = lax.optimization_barrier(jnp.sum(counts, axis=0))
    level_variance = lax.optimization_barrier(jnp.sum(squares, axis=0)) / ((MEMBERS - 1) * COLS)
    bin_corr = bin_sum / jnp.maximum(bin_count, 1.0)[None, :]
    bin_avg = lax.optimization_barrier(jnp.sum(level_variance[:, None] * bin_corr, axis=0)) / jnp.sum(level_variance)
    return (level_variance, bin_corr, bin_avg)
```

```python
import functools

import jax
import jax.numpy as jnp
from jax import lax
from jax.experimental import pallas as pl
from jax.experimental.pallas import tpu as pltpu
from jax.sharding import PartitionSpec as P

BIN_DEV = 8
LANES = 128
PAIR_CHUNK = 512
HALO_CHUNKS = 2


def pieces3(x):
    a = x.astype(jnp.bfloat16).astype(jnp.float32)
    r = x - a
    b = r.astype(jnp.bfloat16).astype(jnp.float32)
    return a, b, r - b


def onehot(rows, base, count):
    ids = lax.broadcasted_iota(jnp.int32, (count, LANES), 0) + base
    parts = [jnp.where(ids == r, 1.0, 0.0) for r in rows]
    return jnp.concatenate(parts, axis=1).astype(jnp.bfloat16)


def perturb(raw, out, squares, width):
    members, lev = raw.shape[0], raw.shape[1]
    rows = members * lev
    for c in range(0, width, LANES):
        cs = pl.ds(c, LANES)
        x = raw[:, :, cs].astype(jnp.float32)
        mean = jnp.sum(x, axis=0) / members
        pert = (x - mean[None]).astype(jnp.bfloat16).astype(jnp.float32)
        sq = jnp.sum(pert * pert, axis=0)
        out[pl.ds(0, rows), cs] = pert.reshape(rows, LANES).astype(jnp.bfloat16)
        inv = 1.0 / jnp.sqrt(sq / (members - 1) + 1e-06)
        hi = inv.astype(jnp.bfloat16).astype(jnp.float32)
        out[pl.ds(rows, 2 * lev), cs] = jnp.concatenate([hi, inv - hi], axis=0).astype(jnp.bfloat16)
        if squares is not None:
            squares[:, cs] = sq


def spread_lanes(x, lev):
    lane = lax.broadcasted_iota(jnp.int32, x.shape, 1)
    s = x + pltpu.roll(x, LANES - lev, 1) + pltpu.roll(x, LANES - 2 * lev, 1)
    s = jnp.where(lane < lev, s, 0.0)
    width = lev
    while width < BIN_DEV * lev:
        s = s + pltpu.roll(s, width, 1)
        width *= 2
    return s


def kernel(
    ntile, nlev, ens, first_in, second_in, bin_in, packed,
    raw, halo, first, second, bins, own, nxt, squares, left_buf, cov_buf, ia_buf, ib_buf,
    bin_hot, parts_buf, bacc, sq_buf, sbuf, rbuf,
    load_sem, halo_send, halo_recv, x_send, x_recv, ready,
):
    members, lev, cols = ens.shape
    rows = members * lev
    half = cols // HALO_CHUNKS
    npairs = bin_hot.shape[1]
    total_bins = BIN_DEV * ntile
    chunks = left_buf.shape[0]
    groups = PAIR_CHUNK // LANES
    me = lax.axis_index("tile")
    my_lev = lax.axis_index("lev")

    barrier = pltpu.get_barrier_semaphore()
    for d in range(1, ntile):
        pl.semaphore_signal(
            barrier, inc=1, device_id=(lax.rem(me + d, ntile), my_lev),
            device_id_type=pl.DeviceIdType.MESH,
        )
    for d in range(1, nlev):
        pl.semaphore_signal(
            barrier, inc=1, device_id=(me, lax.rem(my_lev + d, nlev)),
            device_id_type=pl.DeviceIdType.MESH,
        )
    loads = [
        pltpu.make_async_copy(s, d, load_sem.at[i])
        for i, (s, d) in enumerate(
            ((ens, raw), (first_in, first), (second_in, second), (bin_in, bins))
        )
    ]
    for c in loads:
        c.start()
    loads[0].wait()
    pl.semaphore_wait(barrier, ntile - 1 + nlev - 1)
    prev = lax.rem(me + ntile - 1, ntile)
    halos = [
        pltpu.make_async_remote_copy(
            src_ref=raw.at[:, :, pl.ds(h * half, half)],
            dst_ref=halo.at[h],
            send_sem=halo_send.at[h],
            recv_sem=halo_recv.at[h],
            device_id=(prev, my_lev),
            device_id_type=pl.DeviceIdType.MESH,
        )
        for h in range(HALO_CHUNKS)
    ]
    for c in halos:
        c.start()
    for d in range(1, nlev):
        pl.semaphore_signal(
            ready, inc=1, device_id=(me, lax.rem(my_lev + d, nlev)),
            device_id_type=pl.DeviceIdType.MESH,
        )
    for c in loads[1:]:
        c.wait()

    perturb(raw, own, squares, cols)

    def index_rows(ref, j):
        return [ref[pl.ds(j * groups + i, 1), :] for i in range(groups)]

    def product(a, b):
        return jnp.sum((a * b).reshape(members, lev, PAIR_CHUNK), axis=0)

    def own_step(j, carry):
        x = own[...]
        left = jnp.dot(x, onehot(index_rows(first, j), 0, cols), preferred_element_type=jnp.float32)
        left_buf[j] = left[:rows]
        right = jnp.dot(x, onehot(index_rows(second, j), 0, cols), preferred_element_type=jnp.float32)
        cov_buf[j] = product(left_buf[j], right[:rows])
        ia_buf[j] = left[rows:rows + lev] + left[rows + lev:]
        ib_buf[j] = right[rows:rows + lev] + right[rows + lev:]
        return carry

    lax.fori_loop(0, chunks, own_step, 0)
    def bin_step(j, carry):
        cs = pl.ds(pl.multiple_of(j * PAIR_CHUNK, PAIR_CHUNK), PAIR_CHUNK)
        bin_hot[:, cs] = onehot(index_rows(bins, j), 0, total_bins)
        return carry

    lax.fori_loop(0, chunks, bin_step, 0)
    parts_buf[...] = jnp.concatenate(
        [jnp.zeros((BIN_DEV * lev, npairs), jnp.float32), jnp.ones((LANES - BIN_DEV * lev, npairs), jnp.float32)], axis=0
    ).astype(jnp.bfloat16)
    sq_parts = jnp.concatenate(
        [*pieces3(squares[...]), jnp.zeros((LANES - 3 * lev, cols), jnp.float32)], axis=0
    ).astype(jnp.bfloat16)
    sq_row = lax.dot_general(
        jnp.ones((16, cols), jnp.bfloat16), sq_parts, (((1,), (1,)), ((), ())),
        preferred_element_type=jnp.float32,
    )[:BIN_DEV]
    sq_buf[...] = spread_lanes(sq_row, lev)
    pl.semaphore_wait(ready, nlev - 1)

    for h in range(HALO_CHUNKS):
        halos[h].wait_recv()
        perturb(halo.at[h], nxt.at[h], None, half)

        def next_step(j, carry):
            oh = onehot(index_rows(second, j), cols + h * half, half)
            right = jnp.dot(nxt[h], oh, preferred_element_type=jnp.float32)
            cov = cov_buf[j] + product(left_buf[j], right[:rows])
            ib = ib_buf[j] + right[rows:rows + lev] + right[rows + lev:]
            if h < HALO_CHUNKS - 1:
                cov_buf[j] = cov
                ib_buf[j] = ib
            else:
                corr = cov * ia_buf[j] * ib / (members - 1)
                parts = jnp.concatenate(
                    [*pieces3(corr), jnp.zeros_like(corr)], axis=0
                ).astype(jnp.bfloat16)
                parts_buf[pl.ds(0, 4 * lev), pl.ds(pl.multiple_of(j * PAIR_CHUNK, PAIR_CHUNK), PAIR_CHUNK)] = parts
            return carry

        lax.fori_loop(0, chunks, next_step, 0, unroll=8)

    bacc[...] = lax.dot_general(
        bin_hot[...], parts_buf[...], (((1,), (1,)), ((), ())), preferred_element_type=jnp.float32
    )
    half_lanes = BIN_DEV * lev
    wide_lane = lax.broadcasted_iota(jnp.int32, (total_bins, LANES), 1)
    wide = jnp.where(wide_lane < half_lanes, spread_lanes(bacc[...], lev), bacc[...])
    lane = lax.broadcasted_iota(jnp.int32, (BIN_DEV, LANES), 1)
    bin_row = lax.broadcasted_iota(jnp.int32, (BIN_DEV, LANES), 0)
    pick = (lax.rem(lane, half_lanes) // lev == bin_row).astype(jnp.float32)
    for t in range(ntile):
        block = wide[t * BIN_DEV:(t + 1) * BIN_DEV] * pick
        sbuf[t, 0:1, :] = jnp.sum(block, axis=0, keepdims=True)
        sbuf[t, 1:2, :] = sq_buf[0:1, :]
    mine = my_lev * ntile + me
    rbuf[mine] = sbuf[me]

    def x_copy(d):
        dl, dt = d // ntile, d % ntile
        peer_t = lax.rem(me + dt, ntile)
        peer_l = lax.rem(my_lev + dl, nlev)
        return pltpu.make_async_remote_copy(
            src_ref=sbuf.at[peer_t], dst_ref=rbuf.at[mine],
            send_sem=x_send.at[d], recv_sem=x_recv.at[mine],
            device_id=(peer_t, peer_l), device_id_type=pl.DeviceIdType.MESH,
        )

    def x_start(d, carry):
        x_copy(d).start()
        return carry

    def x_wait_send(d, carry):
        x_copy(d).wait_send()
        return carry

    def x_wait(d, carry):
        src = lax.rem(my_lev + d // ntile, nlev) * ntile + lax.rem(me + d % ntile, ntile)
        pltpu.make_async_copy(rbuf.at[src], rbuf.at[src], x_recv.at[src]).wait()
        return carry

    everyone = ntile * nlev
    small = everyone <= 64
    lax.fori_loop(1, everyone, x_start, 0, unroll=small)
    lax.fori_loop(1, everyone, x_wait, 0, unroll=small)
    num = jnp.zeros((1, LANES), jnp.float32)
    den = num
    own_lv = num
    own_bc = num
    for v in range(nlev):
        tot = rbuf[v * ntile]
        for t in range(1, ntile):
            tot = tot + rbuf[v * ntile + t]
        sums, lv = tot[0:1], tot[1:2] / ((members - 1) * cols * ntile)
        bc = sums / jnp.maximum(pltpu.roll(sums, LANES - half_lanes, 1), 1.0)
        num = num + lv * bc
        den = den + lv
        own_lv = jnp.where(my_lev == v, lv, own_lv)
        own_bc = jnp.where(my_lev == v, bc, own_bc)
    for i, row in enumerate((own_lv, own_bc, num, den)):
        packed[i:i + 1, :] = row

    for c in halos:
        c.wait_send()
    lax.fori_loop(1, everyone, x_wait_send, 0, unroll=small)


def unpack(packed, lv_out, corr_out, avg_out):
    lev = corr_out.shape[0]
    lane = lax.broadcasted_iota(jnp.int32, (BIN_DEV, LANES), 1)
    bin_row = lax.broadcasted_iota(jnp.int32, (BIN_DEV, LANES), 0)

    def by_bin(row):
        x = jnp.where(lane // lev == bin_row, row, 0.0)
        return jnp.sum(jnp.transpose(x).reshape(LANES // lev, lev, BIN_DEV), axis=0)

    lv_out[...] = packed[0:1, :lev]
    corr_out[...] = by_bin(packed[1:2, :])
    num = jnp.sum(by_bin(packed[2:3, :]), axis=0, keepdims=True)
    den = jnp.sum(by_bin(packed[3:4, :]), axis=0, keepdims=True)
    avg_out[...] = num / den


def local(ntile, nlev, ensemble, pair_first, pair_second, pair_bin):
    members, lev, cols = ensemble.shape
    npairs = pair_first.shape[0]
    rows = members * lev
    half = cols // HALO_CHUNKS
    chunks = npairs // PAIR_CHUNK
    total_bins = BIN_DEV * ntile
    f32, bf16 = jnp.float32, jnp.bfloat16
    idx = [x.reshape(npairs // LANES, LANES) for x in (pair_first, pair_second, pair_bin)]
    vmem = pl.BlockSpec(memory_space=pltpu.VMEM)
    hbm = pl.BlockSpec(memory_space=pl.ANY)
    packed = pl.pallas_call(
        functools.partial(kernel, ntile, nlev),
        out_shape=jax.ShapeDtypeStruct((8, LANES), f32),
        in_specs=[hbm] * 4,
        out_specs=vmem,
        scratch_shapes=[
            pltpu.VMEM((members, lev, cols), bf16),
            pltpu.VMEM((HALO_CHUNKS, members, lev, half), bf16),
            *[pltpu.VMEM((npairs // LANES, LANES), jnp.int32)] * 3,
            pltpu.VMEM((rows + 2 * lev, cols), bf16),
            pltpu.VMEM((HALO_CHUNKS, rows + 2 * lev, half), bf16),
            pltpu.VMEM((lev, cols), f32),
            pltpu.VMEM((chunks, rows, PAIR_CHUNK), f32),
            *[pltpu.VMEM((chunks, lev, PAIR_CHUNK), f32)] * 3,
            pltpu.VMEM((total_bins, npairs), bf16),
            pltpu.VMEM((LANES, npairs), bf16),
            pltpu.VMEM((total_bins, LANES), f32),
            pltpu.VMEM((BIN_DEV, LANES), f32),
            pltpu.VMEM((ntile, 2, LANES), f32),
            pltpu.VMEM((nlev * ntile, 2, LANES), f32),
            pltpu.SemaphoreType.DMA((4,)),
            pltpu.SemaphoreType.DMA((HALO_CHUNKS,)),
            pltpu.SemaphoreType.DMA((HALO_CHUNKS,)),
            pltpu.SemaphoreType.DMA((nlev * ntile,)),
            pltpu.SemaphoreType.DMA((nlev * ntile,)),
            pltpu.SemaphoreType.REGULAR,
        ],
        compiler_params=pltpu.CompilerParams(
            collective_id=0, has_side_effects=True, vmem_limit_bytes=55220 * 1024
        ),
        name="binned_corr",
    )(ensemble, *idx)
    lv, corr, avg = pl.pallas_call(
        unpack,
        out_shape=(
            jax.ShapeDtypeStruct((1, lev), f32),
            jax.ShapeDtypeStruct((lev, BIN_DEV), f32),
            jax.ShapeDtypeStruct((1, BIN_DEV), f32),
        ),
        in_specs=[vmem],
        out_specs=(vmem, vmem, vmem),
        compiler_params=pltpu.CompilerParams(vmem_limit_bytes=4 * 1024 * 1024),
        name="unpack",
    )(packed)
    return lv.reshape(lev), corr, avg.reshape(BIN_DEV)


def solution(mesh):
    in_specs = (P(None, "lev", "tile"), P("tile"), P("tile"), P("tile"))
    out_specs = (P("lev"), P("lev", "tile"), P("tile"))
    body = functools.partial(local, mesh.shape["tile"], mesh.shape["lev"])
    return jax.shard_map(body, mesh=mesh, in_specs=in_specs, out_specs=out_specs, check_vma=False)
```

```python
import functools

import jax
import jax.numpy as jnp
from jax import lax
from jax.experimental import pallas as pl
from jax.experimental.pallas import tpu as pltpu
from jax.sharding import PartitionSpec as P

BIN_DEV = 8
LANES = 128
PAIR_CHUNK = 512
SLOTS = LANES // BIN_DEV
MESH = pl.DeviceIdType.MESH


def pieces3(x):
    a = x.astype(jnp.bfloat16).astype(jnp.float32)
    r = x - a
    b = r.astype(jnp.bfloat16).astype(jnp.float32)
    return a, b, r - b


def onehot(rows, base, count):
    ids = lax.broadcasted_iota(jnp.int32, (count, LANES), 0) + base
    parts = [jnp.where(ids == r, 1.0, 0.0) for r in rows]
    return jnp.concatenate(parts, axis=1).astype(jnp.bfloat16)


def inverse_spread(sq, members):
    inv = 1.0 / jnp.sqrt(sq / (members - 1) + 1e-06)
    hi = inv.astype(jnp.bfloat16).astype(jnp.float32)
    return jnp.concatenate([hi, inv - hi], axis=0).astype(jnp.bfloat16)


def perturb(raw, out, squares, c):
    members, lev = raw.shape[0], raw.shape[1]
    rows = members * lev
    cs = pl.ds(c, LANES)
    x = raw[:, :, cs].astype(jnp.float32)
    mean = jnp.sum(x, axis=0) / members
    pert = (x - mean[None]).astype(jnp.bfloat16).astype(jnp.float32)
    sq = jnp.sum(pert * pert, axis=0)
    out[pl.ds(0, rows), cs] = pert.reshape(rows, LANES).astype(jnp.bfloat16)
    out[pl.ds(rows, 2 * lev), cs] = inverse_spread(sq, members)
    squares[:, cs] = sq


def sum_squares(table, first, last, lev):
    x = table[pl.ds(first, last - first), :].astype(jnp.float32)
    return jnp.sum((x * x).reshape((last - first) // lev, lev, x.shape[1]), axis=0)


def flatten(x, tile, shift):
    first = tile // SLOTS * LANES
    turn = (shift - BIN_DEV * (tile % SLOTS)) % LANES
    rest = turn if turn + BIN_DEV * (x.shape[0] - 1) >= LANES else 0
    y = pltpu.roll(x[:, first:first + LANES], turn - rest, 1, stride=BIN_DEV, stride_axis=0)
    if rest:
        y = pltpu.roll(y, rest, 1)
    slot = lax.broadcasted_iota(jnp.int32, y.shape, 1) // BIN_DEV
    level = lax.broadcasted_iota(jnp.int32, y.shape, 0)
    return jnp.sum(jnp.where(slot == level + shift // BIN_DEV, y, 0.0), axis=0, keepdims=True)


def kernel(
    ntile, nlev, ens, first_in, second_in, bin_in, packed,
    raw, own, halo, lst, plst, squares, right_buf, cov_buf, ia_buf, ib_buf,
    hot_buf, bin_hot, pbin_hot, parts_buf, base_buf, count_buf, sbuf, rbuf,
    load_sem, halo_send, halo_recv, list_send, list_recv, x_send, x_recv, ready,
):
    members, lev, cols = ens.shape
    rows = members * lev
    half = cols // 2
    blocks = cols // LANES
    total_bins, npairs = bin_hot.shape
    chunks = npairs // PAIR_CHUNK
    groups = PAIR_CHUNK // LANES
    cut = members * 3 // 5 // 2 * 2 * lev
    me = lax.axis_index("tile")
    my_lev = lax.axis_index("lev")
    after = lax.rem(me + 1, ntile)

    barrier = pltpu.get_barrier_semaphore()
    for d in range(1, ntile):
        pl.semaphore_signal(
            barrier, inc=1, device_id=(lax.rem(me + d, ntile), my_lev), device_id_type=MESH
        )
    for d in range(1, nlev):
        pl.semaphore_signal(
            barrier, inc=1, device_id=(me, lax.rem(my_lev + d, nlev)), device_id_type=MESH
        )
    loads = [
        pltpu.make_async_copy(
            ens.at[:, :, pl.ds(c * LANES, LANES)], raw.at[:, :, pl.ds(c * LANES, LANES)], load_sem.at[c]
        )
        for c in range(blocks)
    ]
    list_loads = [
        pltpu.make_async_copy(s, lst.at[i], load_sem.at[blocks + i])
        for i, s in enumerate((first_in, second_in, bin_in))
    ]
    for c in loads[:1] + list_loads + loads[1:]:
        c.start()

    share = lst.shape[1] // nlev
    quarter = pl.ds(pl.multiple_of(my_lev * share, share), share)

    def list_copy(d):
        peer = (me, lax.rem(my_lev + d, nlev)) if d else (after, my_lev)
        src = plst if d else lst
        return pltpu.make_async_remote_copy(
            src_ref=src.at[:, quarter, :], dst_ref=plst.at[:, quarter, :],
            send_sem=list_send.at[d], recv_sem=list_recv.at[my_lev],
            device_id=peer, device_id_type=MESH,
        )

    def piece(i, dst, src_rows, src_cols):
        return pltpu.make_async_remote_copy(
            src_ref=own.at[src_rows, src_cols], dst_ref=dst,
            send_sem=halo_send.at[i], recv_sem=halo_recv.at[i],
            device_id=(after, my_lev), device_id_type=MESH,
        )

    near = half // LANES
    halos = [
        piece(c, halo.at[0, pl.ds(0, rows), pl.ds(c * LANES, LANES)], pl.ds(0, rows), pl.ds(c * LANES, LANES))
        for c in range(near)
    ]
    halos.append(piece(near, halo.at[1, pl.ds(0, cut), :], pl.ds(0, cut), pl.ds(half, half)))
    halos.append(piece(near + 1, halo.at[1, pl.ds(cut, rows - cut), :], pl.ds(cut, rows - cut), pl.ds(half, half)))

    loads[0].wait()
    perturb(raw, own, squares, 0)
    for c in list_loads:
        c.wait()
    pl.semaphore_wait(barrier, ntile - 1 + nlev - 1)
    list_copy(0).start()
    halos[0].start()
    for c in range(1, blocks):
        loads[c].wait()
        perturb(raw, own, squares, c * LANES)
        if c < near:
            halos[c].start()
    halos[near].start()
    halos[near + 1].start()
    for d in range(1, nlev):
        pl.semaphore_signal(
            ready, inc=1, device_id=(me, lax.rem(my_lev + d, nlev)), device_id_type=MESH
        )

    def index_rows(ref, i, j):
        return [ref[i, pl.ds(j * groups + g, 1), :] for g in range(groups)]

    def pairs(j):
        return pl.ds(pl.multiple_of(j * PAIR_CHUNK, PAIR_CHUNK), PAIR_CHUNK)

    def product(a, b):
        return jnp.sum((a * b).reshape(a.shape[0] // lev, lev, PAIR_CHUNK), axis=0)

    def two(x):
        return x[:lev] + x[lev:]

    def corr_parts(cov, ia, ib, last):
        corr = cov * ia * ib / (members - 1)
        return jnp.concatenate([*pieces3(corr), jnp.full_like(corr, last)], axis=0).astype(jnp.bfloat16)

    def gather(table, hot):
        return jnp.dot(table, hot, preferred_element_type=jnp.float32)

    def own_step(j, carry):
        x = own[...]
        left = gather(x, onehot(index_rows(lst, 0, j), 0, cols))
        right = gather(x, onehot(index_rows(lst, 1, j), 0, cols))
        parts_buf[:, pairs(j)] = corr_parts(
            product(left[:rows], right[:rows]), two(left[rows:]), two(right[rows:]), 1.0
        )
        bin_hot[:, pairs(j)] = onehot(index_rows(lst, 2, j), 0, total_bins)
        return carry

    lax.fori_loop(0, chunks // 2, own_step, 0)
    list_copy(0).wait_recv()
    for d in range(1, nlev):
        list_copy(d).start()
    lax.fori_loop(chunks // 2, chunks, own_step, 0)

    def bin_dot(parts, hot):
        return lax.dot_general(
            parts, hot, (((1,), (1,)), ((), ())), preferred_element_type=jnp.float32
        )

    def bin_sums(x):
        return x[:lev] + x[lev:2 * lev] + x[2 * lev:3 * lev]

    binned = bin_dot(parts_buf[...], bin_hot[...])
    base_buf[...] = bin_sums(binned)
    counts = binned[3 * lev:]
    lane = lax.broadcasted_iota(jnp.int32, (lev, LANES), 1)
    level = lax.broadcasted_iota(jnp.int32, (lev, LANES), 0)
    level_squares = jnp.sum(
        jnp.where(lane // BIN_DEV == level + SLOTS // 2, jnp.sum(squares[...], axis=1, keepdims=True), 0.0), axis=0, keepdims=True
    )
    for t in range(ntile):
        sbuf[t, 1:2, :] = level_squares
        count_buf[t] = flatten(counts, t, 0)

    for d in range(1, nlev):
        src = lax.rem(my_lev + d, nlev)
        part = plst.at[:, pl.ds(pl.multiple_of(src * share, share), share), :]
        pltpu.make_async_copy(part, part, list_recv.at[src]).wait()

    def cross_step(j, carry):
        oh = onehot([r - cols for r in index_rows(plst, 1, j)], 0, cols)
        right = gather(own[...], oh)
        right_buf[j] = right[:rows]
        ib_buf[j] = two(right[rows:])
        pbin_hot[:, pairs(j)] = onehot(index_rows(plst, 2, j), 0, total_bins)
        hot_buf[:, pairs(j)] = onehot(index_rows(plst, 0, j), half, half)
        return carry

    lax.fori_loop(0, chunks, cross_step, 0)
    pl.semaphore_wait(ready, nlev - 1)

    for c in range(near):
        halos[c].wait_recv()
    halo[0, pl.ds(rows, 2 * lev), :] = inverse_spread(sum_squares(halo.at[0], 0, rows, lev), members)

    def near_step(j, carry):
        left = gather(halo[0], onehot(index_rows(plst, 0, j), 0, half))
        cov_buf[j] = product(left[:rows], right_buf[j])
        ia_buf[j] = two(left[rows:])
        return carry

    lax.fori_loop(0, chunks, near_step, 0)

    halos[near].wait_recv()
    far = sum_squares(halo.at[1], 0, cut, lev)

    def mid_step(j, carry):
        left = gather(halo[1, pl.ds(0, cut), :], hot_buf[:, pairs(j)])
        cov_buf[j] = cov_buf[j] + product(left, right_buf[j, pl.ds(0, cut), :])
        return carry

    lax.fori_loop(0, chunks, mid_step, 0)

    halos[near + 1].wait_recv()
    far = far + sum_squares(halo.at[1], cut, rows, lev)
    halo[1, pl.ds(rows, 2 * lev), :] = inverse_spread(far, members)

    kept = rows - cut

    def far_step(j, total):
        left = gather(halo[1, pl.ds(cut, kept + 2 * lev), :], hot_buf[:, pairs(j)])
        cov = cov_buf[j] + product(left[:kept], right_buf[j, pl.ds(cut, kept), :])
        ia = ia_buf[j] + two(left[kept:])
        return total + bin_dot(corr_parts(cov, ia, ib_buf[j], 0.0), pbin_hot[:, pairs(j)])

    total = lax.fori_loop(0, chunks, far_step, jnp.zeros((4 * lev, total_bins), jnp.float32), unroll=True)
    sums = base_buf[...] + bin_sums(total)
    for t in range(ntile):
        sbuf[t, 0:1, :] = flatten(sums, t, LANES // 2) + count_buf[t]
    mine = my_lev * ntile + me

    def x_copy(d):
        dl, dt = d // ntile, d % ntile
        peer_t = lax.rem(me + dt, ntile)
        peer_l = lax.rem(my_lev + dl, nlev)
        return pltpu.make_async_remote_copy(
            src_ref=sbuf.at[peer_t], dst_ref=rbuf.at[mine],
            send_sem=x_send.at[d], recv_sem=x_recv.at[mine],
            device_id=(peer_t, peer_l), device_id_type=MESH,
        )

    def x_start(d, carry):
        x_copy(d).start()
        return carry

    def x_wait_send(d, carry):
        x_copy(d).wait_send()
        return carry

    def x_wait(d, carry):
        src = lax.rem(my_lev + d // ntile, nlev) * ntile + lax.rem(me + d % ntile, ntile)
        pltpu.make_async_copy(rbuf.at[src], rbuf.at[src], x_recv.at[src]).wait()
        return carry

    everyone = ntile * nlev
    small = everyone <= 64
    lax.fori_loop(1, everyone, x_start, 0, unroll=small)
    rbuf[mine] = sbuf[me]
    for c in halos:
        c.wait_send()
    for d in range(nlev):
        list_copy(d).wait_send()
    lax.fori_loop(1, everyone, x_wait, 0, unroll=small)
    num = jnp.zeros((1, LANES), jnp.float32)
    den = num
    own_lv = num
    own_bc = num
    for v in range(nlev):
        tot = rbuf[v * ntile]
        for t in range(1, ntile):
            tot = tot + rbuf[v * ntile + t]
        sums, lv = tot[0:1], tot[1:2] / ((members - 1) * cols * ntile)
        bc = sums / jnp.maximum(pltpu.roll(sums, LANES // 2, 1), 1.0)
        num = num + lv * bc
        den = den + lv
        own_lv = jnp.where(my_lev == v, lv, own_lv)
        own_bc = jnp.where(my_lev == v, bc, own_bc)

    def by_level(row):
        turn = LANES // 2 - BIN_DEV * (lev - 1)
        return pltpu.roll(jnp.broadcast_to(row, (lev, LANES)), turn, 1, stride=BIN_DEV, stride_axis=0)

    corr = by_level(own_bc)
    for v in range(lev):
        packed[v:v + 1, :] = corr[lev - 1 - v:lev - v]
    diagonal = lane + level == lev - 1
    packed[lev:lev + 1, :] = jnp.sum(jnp.where(diagonal, by_level(own_lv), 0.0), axis=0, keepdims=True)
    packed[lev + 1:lev + 2, :] = jnp.sum(by_level(num), axis=0, keepdims=True) / jnp.sum(
        by_level(den), axis=0, keepdims=True
    )
    lax.fori_loop(1, everyone, x_wait_send, 0, unroll=small)


def unpack(packed, lv_out, corr_out, avg_out):
    lev = corr_out.shape[0]
    corr_out[...] = packed[0:lev, :BIN_DEV]
    lv_out[...] = packed[lev:lev + 1, :lev]
    avg_out[...] = packed[lev + 1:lev + 2, :BIN_DEV]


def local(ntile, nlev, ensemble, pair_first, pair_second, pair_bin):
    members, lev, cols = ensemble.shape
    npairs = pair_first.shape[0]
    rows = members * lev
    half = cols // 2
    pieces = half // LANES + 2
    chunks = npairs // PAIR_CHUNK
    total_bins = -(-BIN_DEV * ntile // LANES) * LANES
    f32, bf16 = jnp.float32, jnp.bfloat16
    idx = [x.reshape(npairs // LANES, LANES) for x in (pair_first, pair_second, pair_bin)]
    vmem = pl.BlockSpec(memory_space=pltpu.VMEM)
    hbm = pl.BlockSpec(memory_space=pl.ANY)
    packed = pl.pallas_call(
        functools.partial(kernel, ntile, nlev),
        out_shape=jax.ShapeDtypeStruct((2 * lev, LANES), f32),
        in_specs=[hbm] * 4,
        out_specs=vmem,
        scratch_shapes=[
            pltpu.VMEM((members, lev, cols), bf16),
            pltpu.VMEM((rows + 2 * lev, cols), bf16),
            pltpu.VMEM((2, rows + 2 * lev, half), bf16),
            pltpu.VMEM((3, npairs // LANES, LANES), jnp.int32),
            pltpu.VMEM((3, npairs // LANES, LANES), jnp.int32),
            pltpu.VMEM((lev, cols), f32),
            pltpu.VMEM((chunks, rows, PAIR_CHUNK), f32),
            *[pltpu.VMEM((chunks, lev, PAIR_CHUNK), f32)] * 3,
            pltpu.VMEM((half, npairs), bf16),
            pltpu.VMEM((total_bins, npairs), bf16),
            pltpu.VMEM((total_bins, npairs), bf16),
            pltpu.VMEM((4 * lev, npairs), bf16),
            pltpu.VMEM((lev, total_bins), f32),
            pltpu.VMEM((ntile, 1, LANES), f32),
            pltpu.VMEM((ntile, 2, LANES), f32),
            pltpu.VMEM((nlev * ntile, 2, LANES), f32),
            pltpu.SemaphoreType.DMA((cols // LANES + 3,)),
            pltpu.SemaphoreType.DMA((pieces,)),
            pltpu.SemaphoreType.DMA((pieces,)),
            pltpu.SemaphoreType.DMA((nlev,)),
            pltpu.SemaphoreType.DMA((nlev,)),
            pltpu.SemaphoreType.DMA((nlev * ntile,)),
            pltpu.SemaphoreType.DMA((nlev * ntile,)),
            pltpu.SemaphoreType.REGULAR,
        ],
        compiler_params=pltpu.CompilerParams(
            collective_id=0, has_side_effects=True, vmem_limit_bytes=55220 * 1024
        ),
        name="binned_corr",
    )(ensemble, *idx)
    lv, corr, avg = pl.pallas_call(
        unpack,
        out_shape=(
            jax.ShapeDtypeStruct((1, lev), f32),
            jax.ShapeDtypeStruct((lev, BIN_DEV), f32),
            jax.ShapeDtypeStruct((1, BIN_DEV), f32),
        ),
        in_specs=[vmem],
        out_specs=(vmem, vmem, vmem),
        compiler_params=pltpu.CompilerParams(vmem_limit_bytes=4 * 1024 * 1024),
        name="unpack",
    )(packed)
    return lv.reshape(lev), corr, avg.reshape(BIN_DEV)


def solution(mesh):
    in_specs = (P(None, "lev", "tile"), P("tile"), P("tile"), P("tile"))
    out_specs = (P("lev"), P("lev", "tile"), P("tile"))
    body = functools.partial(local, mesh.shape["tile"], mesh.shape["lev"])
    return jax.shard_map(body, mesh=mesh, in_specs=in_specs, out_specs=out_specs, check_vma=False)
```

```python
import functools

import jax
import jax.numpy as jnp
from jax import lax
from jax.experimental import pallas as pl
from jax.experimental.pallas import tpu as pltpu
from jax.sharding import PartitionSpec as P

BIN_DEV = 8
LANES = 128
PAIR_CHUNK = 512
SLOTS = LANES // BIN_DEV
OWN, CROSS, NEAR, MID = 2, 4, 8, 8
CUTS = (12, 16)
MESH = pl.DeviceIdType.MESH


def pieces3(x):
    a = x.astype(jnp.bfloat16).astype(jnp.float32)
    r = x - a
    b = r.astype(jnp.bfloat16).astype(jnp.float32)
    return a, b, r - b


def onehot(rows, base, count):
    ids = lax.broadcasted_iota(jnp.int32, (count, LANES), 0) + base
    parts = [jnp.where(ids == r, 1.0, 0.0) for r in rows]
    return jnp.concatenate(parts, axis=1).astype(jnp.bfloat16)


def inverse_spread(sq, members):
    inv = 1.0 / jnp.sqrt(sq / (members - 1) + 1e-06)
    hi = inv.astype(jnp.bfloat16).astype(jnp.float32)
    return jnp.concatenate([hi, inv - hi], axis=0).astype(jnp.bfloat16)


def perturb(raw, out, squares, c):
    members, lev = raw.shape[0], raw.shape[1]
    rows = members * lev
    cs = pl.ds(c, LANES)
    x = raw[:, :, cs].astype(jnp.float32)
    mean = jnp.sum(x, axis=0) / members
    pert = (x - mean[None]).astype(jnp.bfloat16).astype(jnp.float32)
    sq = jnp.sum(pert * pert, axis=0)
    out[pl.ds(0, rows), cs] = pert.reshape(rows, LANES).astype(jnp.bfloat16)
    out[pl.ds(rows, 2 * lev), cs] = inverse_spread(sq, members)
    squares[:, cs] = sq


def sum_squares(table, first, last, lev):
    x = table[pl.ds(first, last - first), :].astype(jnp.float32)
    return jnp.sum((x * x).reshape((last - first) // lev, lev, x.shape[1]), axis=0)


def flatten(x, tile, shift):
    first = tile // SLOTS * LANES
    turn = (shift - BIN_DEV * (tile % SLOTS)) % LANES
    rest = turn if turn + BIN_DEV * (x.shape[0] - 1) >= LANES else 0
    y = pltpu.roll(x[:, first:first + LANES], turn - rest, 1, stride=BIN_DEV, stride_axis=0)
    if rest:
        y = pltpu.roll(y, rest, 1)
    slot = lax.broadcasted_iota(jnp.int32, y.shape, 1) // BIN_DEV
    level = lax.broadcasted_iota(jnp.int32, y.shape, 0)
    return jnp.sum(jnp.where(slot == level + shift // BIN_DEV, y, 0.0), axis=0, keepdims=True)


def kernel(
    ntile, nlev, ens, first_in, second_in, bin_in, packed,
    raw, own, halo, lst, plst, squares, right_buf, cov_buf, ia_buf, ib_buf,
    bin_hot, parts_buf, base_buf, wide_buf, count_buf, sbuf, rbuf,
    load_sem, halo_send, halo_recv, list_send, list_recv, x_send, x_recv, ready,
):
    members, lev, cols = ens.shape
    rows = members * lev
    half = cols // 2
    blocks = cols // LANES
    total_bins, npairs = bin_hot.shape
    chunks = npairs // PAIR_CHUNK
    groups = PAIR_CHUNK // LANES
    cuts = [0] + [members * n // 20 // 2 * 2 * lev for n in CUTS] + [rows]
    me = lax.axis_index("tile")
    my_lev = lax.axis_index("lev")
    after = lax.rem(me + 1, ntile)

    barrier = pltpu.get_barrier_semaphore()
    for d in range(1, ntile):
        pl.semaphore_signal(
            barrier, inc=1, device_id=(lax.rem(me + d, ntile), my_lev), device_id_type=MESH
        )
    for d in range(1, nlev):
        pl.semaphore_signal(
            barrier, inc=1, device_id=(me, lax.rem(my_lev + d, nlev)), device_id_type=MESH
        )
    loads = [
        pltpu.make_async_copy(
            ens.at[:, :, pl.ds(c * LANES, LANES)], raw.at[:, :, pl.ds(c * LANES, LANES)], load_sem.at[c]
        )
        for c in range(blocks)
    ]
    list_loads = [
        pltpu.make_async_copy(s, lst.at[i], load_sem.at[blocks + i])
        for i, s in enumerate((first_in, second_in, bin_in))
    ]
    for c in loads[:1] + list_loads + loads[1:]:
        c.start()

    share = lst.shape[1] // nlev
    quarter = pl.ds(pl.multiple_of(my_lev * share, share), share)

    def list_copy(d):
        peer = (me, lax.rem(my_lev + d, nlev)) if d else (after, my_lev)
        src = plst if d else lst
        return pltpu.make_async_remote_copy(
            src_ref=src.at[:, quarter, :], dst_ref=plst.at[:, quarter, :],
            send_sem=list_send.at[d], recv_sem=list_recv.at[my_lev],
            device_id=peer, device_id_type=MESH,
        )

    def piece(i, dst, src_rows, src_cols):
        return pltpu.make_async_remote_copy(
            src_ref=own.at[src_rows, src_cols], dst_ref=dst,
            send_sem=halo_send.at[i], recv_sem=halo_recv.at[i],
            device_id=(after, my_lev), device_id_type=MESH,
        )

    near = half // LANES
    halos = [
        piece(c, halo.at[0, pl.ds(0, rows), pl.ds(c * LANES, LANES)], pl.ds(0, rows), pl.ds(c * LANES, LANES))
        for c in range(near)
    ]
    spans = list(zip(cuts[:-1], cuts[1:]))
    for i, (a, b) in enumerate(spans):
        halos.append(piece(near + i, halo.at[1, pl.ds(a, b - a), :], pl.ds(a, b - a), pl.ds(half, half)))

    loads[0].wait()
    perturb(raw, own, squares, 0)
    for c in list_loads:
        c.wait()
    pl.semaphore_wait(barrier, ntile - 1 + nlev - 1)
    list_copy(0).start()
    halos[0].start()
    for c in range(1, blocks):
        loads[c].wait()
        perturb(raw, own, squares, c * LANES)
        if c < near:
            halos[c].start()
    for c in halos[near:]:
        c.start()
    for d in range(1, nlev):
        pl.semaphore_signal(
            ready, inc=1, device_id=(me, lax.rem(my_lev + d, nlev)), device_id_type=MESH
        )

    def index_rows(ref, i, j):
        return [ref[i, pl.ds(j * groups + g, 1), :] for g in range(groups)]

    def pairs(j):
        return pl.ds(pl.multiple_of(j * PAIR_CHUNK, PAIR_CHUNK), PAIR_CHUNK)

    def product(a, b):
        return jnp.sum((a * b).reshape(a.shape[0] // lev, lev, PAIR_CHUNK), axis=0)

    def two(x):
        return x[:lev] + x[lev:]

    def corr_parts(cov, ia, ib, last):
        corr = cov * ia * ib / (members - 1)
        return jnp.concatenate([*pieces3(corr), jnp.full_like(corr, last)], axis=0).astype(jnp.bfloat16)

    def gather(table, hot):
        return jnp.dot(table, hot, preferred_element_type=jnp.float32)

    def own_step(j, carry):
        x = own[...]
        left = gather(x, onehot(index_rows(lst, 0, j), 0, cols))
        right = gather(x, onehot(index_rows(lst, 1, j), 0, cols))
        parts_buf[:, pairs(j)] = corr_parts(
            product(left[:rows], right[:rows]), two(left[rows:]), two(right[rows:]), 1.0
        )
        bin_hot[:, pairs(j)] = onehot(index_rows(lst, 2, j), 0, total_bins)
        return carry

    lax.fori_loop(0, chunks // 2, own_step, 0, unroll=OWN)
    list_copy(0).wait_recv()
    for d in range(1, nlev):
        list_copy(d).start()
    lax.fori_loop(chunks // 2, chunks, own_step, 0, unroll=OWN)

    def bin_dot(parts, hot):
        return lax.dot_general(
            parts, hot, (((1,), (1,)), ((), ())), preferred_element_type=jnp.float32
        )

    def bin_sums(x):
        return x[:lev] + x[lev:2 * lev] + x[2 * lev:3 * lev]

    binned = bin_dot(parts_buf[...], bin_hot[...])
    base_buf[...] = bin_sums(binned)
    wide_buf[...] = jnp.zeros_like(wide_buf)
    wide_buf[0, :, pl.ds(0, total_bins)] = binned[3 * lev:]
    counts = wide_buf[0]
    lane = lax.broadcasted_iota(jnp.int32, (lev, LANES), 1)
    level = lax.broadcasted_iota(jnp.int32, (lev, LANES), 0)
    level_squares = jnp.sum(
        jnp.where(lane // BIN_DEV == level + SLOTS // 2, jnp.sum(squares[...], axis=1, keepdims=True), 0.0), axis=0, keepdims=True
    )
    for t in range(ntile):
        sbuf[t, 1:2, :] = level_squares
        count_buf[t] = flatten(counts, t, 0)

    for d in range(1, nlev):
        src = lax.rem(my_lev + d, nlev)
        part = plst.at[:, pl.ds(pl.multiple_of(src * share, share), share), :]
        pltpu.make_async_copy(part, part, list_recv.at[src]).wait()

    def cross_step(j, carry):
        oh = onehot([r - cols for r in index_rows(plst, 1, j)], 0, cols)
        right = gather(own[...], oh)
        right_buf[j] = right[:rows]
        ib_buf[j] = two(right[rows:])
        return carry

    lax.fori_loop(0, chunks, cross_step, 0, unroll=CROSS)
    pl.semaphore_wait(ready, nlev - 1)

    for c in range(near):
        halos[c].wait_recv()
    halo[0, pl.ds(rows, 2 * lev), :] = inverse_spread(sum_squares(halo.at[0], 0, rows, lev), members)

    def near_step(j, carry):
        left = gather(halo[0], onehot(index_rows(plst, 0, j), 0, half))
        cov_buf[j] = product(left[:rows], right_buf[j])
        ia_buf[j] = two(left[rows:])
        return carry

    lax.fori_loop(0, chunks, near_step, 0, unroll=NEAR)

    far = jnp.zeros((lev, half), jnp.float32)
    for i, (a, b) in enumerate(spans[:-1]):
        halos[near + i].wait_recv()
        far = far + sum_squares(halo.at[1], a, b, lev)

        def mid_step(j, carry):
            left = gather(halo[1, pl.ds(a, b - a), :], onehot(index_rows(plst, 0, j), half, half))
            cov_buf[j] = cov_buf[j] + product(left, right_buf[j, pl.ds(a, b - a), :])
            return carry

        lax.fori_loop(0, chunks, mid_step, 0, unroll=MID)

    cut = cuts[-2]
    halos[-1].wait_recv()
    far = far + sum_squares(halo.at[1], cut, rows, lev)
    halo[1, pl.ds(rows, 2 * lev), :] = inverse_spread(far, members)

    kept = rows - cut

    def far_step(j, total):
        left = gather(halo[1, pl.ds(cut, kept + 2 * lev), :], onehot(index_rows(plst, 0, j), half, half))
        cov = cov_buf[j] + product(left[:kept], right_buf[j, pl.ds(cut, kept), :])
        ia = ia_buf[j] + two(left[kept:])
        return total + bin_dot(corr_parts(cov, ia, ib_buf[j], 0.0), onehot(index_rows(plst, 2, j), 0, total_bins))

    total = lax.fori_loop(0, chunks, far_step, jnp.zeros((4 * lev, total_bins), jnp.float32), unroll=True)
    wide_buf[1, :, pl.ds(0, total_bins)] = base_buf[...] + bin_sums(total)
    sums = wide_buf[1]
    for t in range(ntile):
        sbuf[t, 0:1, :] = flatten(sums, t, LANES // 2) + count_buf[t]
    mine = my_lev * ntile + me

    def x_start(d, carry):
        dl, dt = d // ntile, d % ntile
        peer_t = lax.rem(me + dt, ntile)
        peer_l = lax.rem(my_lev + dl, nlev)
        pltpu.make_async_remote_copy(
            src_ref=sbuf.at[peer_t], dst_ref=rbuf.at[mine],
            send_sem=x_send.at[0], recv_sem=x_recv.at[0],
            device_id=(peer_t, peer_l), device_id_type=MESH,
        ).start()
        return carry

    def x_wait(sem):
        rest = rbuf.at[pl.ds(0, everyone - 1)]
        pltpu.make_async_copy(rest, rest, sem).wait()

    everyone = ntile * nlev
    small = everyone <= 64
    lax.fori_loop(1, everyone, x_start, 0, unroll=small)
    rbuf[mine] = sbuf[me]
    for c in halos:
        c.wait_send()
    for d in range(nlev):
        list_copy(d).wait_send()
    x_wait(x_send.at[0])
    x_wait(x_recv.at[0])
    num = jnp.zeros((1, LANES), jnp.float32)
    den = num
    own_lv = num
    own_bc = num
    for v in range(nlev):
        tot = rbuf[v * ntile]
        for t in range(1, ntile):
            tot = tot + rbuf[v * ntile + t]
        sums, lv = tot[0:1], tot[1:2] / ((members - 1) * cols * ntile)
        bc = sums / jnp.maximum(pltpu.roll(sums, LANES // 2, 1), 1.0)
        num = num + lv * bc
        den = den + lv
        own_lv = jnp.where(my_lev == v, lv, own_lv)
        own_bc = jnp.where(my_lev == v, bc, own_bc)

    def by_level(row):
        turn = LANES // 2 - BIN_DEV * (lev - 1)
        return pltpu.roll(jnp.broadcast_to(row, (lev, LANES)), turn, 1, stride=BIN_DEV, stride_axis=0)

    corr = by_level(own_bc)
    for v in range(lev):
        packed[v:v + 1, :] = corr[lev - 1 - v:lev - v]
    diagonal = lane + level == lev - 1
    packed[lev:lev + 1, :] = jnp.sum(jnp.where(diagonal, by_level(own_lv), 0.0), axis=0, keepdims=True)
    packed[lev + 1:lev + 2, :] = jnp.sum(by_level(num), axis=0, keepdims=True) / jnp.sum(
        by_level(den), axis=0, keepdims=True
    )


def unpack(packed, lv_out, corr_out, avg_out):
    lev = corr_out.shape[0]
    corr_out[...] = packed[0:lev, :BIN_DEV]
    lv_out[...] = packed[lev:lev + 1, :lev]
    avg_out[...] = packed[lev + 1:lev + 2, :BIN_DEV]


def local(ntile, nlev, ensemble, pair_first, pair_second, pair_bin):
    members, lev, cols = ensemble.shape
    npairs = pair_first.shape[0]
    rows = members * lev
    half = cols // 2
    pieces = half // LANES + len(CUTS) + 1
    chunks = npairs // PAIR_CHUNK
    total_bins = BIN_DEV * ntile
    bin_lanes = -(-total_bins // LANES) * LANES
    f32, bf16 = jnp.float32, jnp.bfloat16
    idx = [x.reshape(npairs // LANES, LANES) for x in (pair_first, pair_second, pair_bin)]
    vmem = pl.BlockSpec(memory_space=pltpu.VMEM)
    hbm = pl.BlockSpec(memory_space=pl.ANY)
    packed = pl.pallas_call(
        functools.partial(kernel, ntile, nlev),
        out_shape=jax.ShapeDtypeStruct((2 * lev, LANES), f32),
        in_specs=[hbm] * 4,
        out_specs=vmem,
        scratch_shapes=[
            pltpu.VMEM((members, lev, cols), bf16),
            pltpu.VMEM((rows + 2 * lev, cols), bf16),
            pltpu.VMEM((2, rows + 2 * lev, half), bf16),
            pltpu.VMEM((3, npairs // LANES, LANES), jnp.int32),
            pltpu.VMEM((3, npairs // LANES, LANES), jnp.int32),
            pltpu.VMEM((lev, cols), f32),
            pltpu.VMEM((chunks, rows, PAIR_CHUNK), f32),
            *[pltpu.VMEM((chunks, lev, PAIR_CHUNK), f32)] * 3,
            pltpu.VMEM((total_bins, npairs), bf16),
            pltpu.VMEM((4 * lev, npairs), bf16),
            pltpu.VMEM((lev, total_bins), f32),
            pltpu.VMEM((2, lev, bin_lanes), f32),
            pltpu.VMEM((ntile, 1, LANES), f32),
            pltpu.VMEM((ntile, 2, LANES), f32),
            pltpu.VMEM((nlev * ntile, 2, LANES), f32),
            pltpu.SemaphoreType.DMA((cols // LANES + 3,)),
            pltpu.SemaphoreType.DMA((pieces,)),
            pltpu.SemaphoreType.DMA((pieces,)),
            pltpu.SemaphoreType.DMA((nlev,)),
            pltpu.SemaphoreType.DMA((nlev,)),
            pltpu.SemaphoreType.DMA((1,)),
            pltpu.SemaphoreType.DMA((1,)),
            pltpu.SemaphoreType.REGULAR,
        ],
        compiler_params=pltpu.CompilerParams(
            collective_id=0, has_side_effects=True, vmem_limit_bytes=55220 * 1024
        ),
        name="binned_corr",
    )(ensemble, *idx)
    lv, corr, avg = pl.pallas_call(
        unpack,
        out_shape=(
            jax.ShapeDtypeStruct((1, lev), f32),
            jax.ShapeDtypeStruct((lev, BIN_DEV), f32),
            jax.ShapeDtypeStruct((1, BIN_DEV), f32),
        ),
        in_specs=[vmem],
        out_specs=(vmem, vmem, vmem),
        compiler_params=pltpu.CompilerParams(vmem_limit_bytes=4 * 1024 * 1024),
        name="unpack",
    )(packed)
    return lv.reshape(lev), corr, avg.reshape(BIN_DEV)


def solution(mesh):
    in_specs = (P(None, "lev", "tile"), P("tile"), P("tile"), P("tile"))
    out_specs = (P("lev"), P("lev", "tile"), P("tile"))
    body = functools.partial(local, mesh.shape["tile"], mesh.shape["lev"])
    return jax.shard_map(body, mesh=mesh, in_specs=in_specs, out_specs=out_specs, check_vma=False)
```

```python
import functools

import jax
import jax.numpy as jnp
from jax import lax
from jax.experimental import pallas as pl
from jax.experimental.pallas import tpu as pltpu
from jax.sharding import PartitionSpec as P

BIN_DEV = 8
LANES = 128
PAIR_CHUNK = 512
SLOTS = LANES // BIN_DEV
OWN, CROSS, NEAR = 2, 4, 8
HOT = jnp.float8_e4m3fn
CUTS = (12, 16)
MESH = pl.DeviceIdType.MESH


def onehot(rows, base, count):
    ids = lax.broadcasted_iota(jnp.int32, (count, LANES), 0) + base
    parts = [jnp.where(ids == r, 1.0, 0.0) for r in rows]
    return jnp.concatenate(parts, axis=1).astype(jnp.bfloat16)


def inverse_spread(sq, members):
    inv = 1.0 / jnp.sqrt(sq / (members - 1) + 1e-06)
    hi = inv.astype(jnp.bfloat16).astype(jnp.float32)
    return jnp.concatenate([hi, inv - hi], axis=0).astype(jnp.bfloat16)


def perturb(raw, out, squares, c):
    members, lev = raw.shape[0], raw.shape[1]
    rows = members * lev
    cs = pl.ds(c, LANES)
    x = raw[:, :, cs].astype(jnp.float32)
    mean = jnp.sum(x, axis=0) / members
    pert = (x - mean[None]).astype(jnp.bfloat16).astype(jnp.float32)
    sq = jnp.sum(pert * pert, axis=0)
    out[pl.ds(0, rows), cs] = pert.reshape(rows, LANES).astype(jnp.bfloat16)
    out[pl.ds(rows, 2 * lev), cs] = inverse_spread(sq, members)
    squares[:, cs] = sq


def sum_squares(table, first, last, col, count, lev):
    x = table[pl.ds(first, last - first), pl.ds(col, count)].astype(jnp.float32)
    return jnp.sum((x * x).reshape((last - first) // lev, lev, x.shape[1]), axis=0)


def flatten(x, tile, shift):
    first = tile // SLOTS * LANES
    turn = (shift - BIN_DEV * (tile % SLOTS)) % LANES
    rest = turn if turn + BIN_DEV * (x.shape[0] - 1) >= LANES else 0
    y = pltpu.roll(x[:, first:first + LANES], turn - rest, 1, stride=BIN_DEV, stride_axis=0)
    if rest:
        y = pltpu.roll(y, rest, 1)
    slot = lax.broadcasted_iota(jnp.int32, y.shape, 1) // BIN_DEV
    level = lax.broadcasted_iota(jnp.int32, y.shape, 0)
    return jnp.sum(jnp.where(slot == level + shift // BIN_DEV, y, 0.0), axis=0, keepdims=True)


def kernel(
    ntile, nlev, ens, first_in, second_in, bin_in, packed,
    raw, own, halo, lst, pack, plst, squares, right_buf, cov_buf, ia_buf, ib_buf,
    hot_buf, bin_hot, pbin_hot, parts_buf, base_buf, wide_buf, early_out, early_in, variance, scale, sbuf, rbuf,
    load_sem, halo_send, halo_recv, list_sem, early_sem, x_sem, ready,
):
    members, lev, cols = ens.shape
    rows = members * lev
    half = cols // 2
    blocks = cols // LANES
    total_bins, npairs = bin_hot.shape
    chunks = npairs // PAIR_CHUNK
    groups = PAIR_CHUNK // LANES
    cuts = [0] + [members * n // 20 // 2 * 2 * lev for n in CUTS] + [rows]
    me = lax.axis_index("tile")
    my_lev = lax.axis_index("lev")
    after = lax.rem(me + 1, ntile)

    barrier = pltpu.get_barrier_semaphore()
    for d in range(1, ntile):
        pl.semaphore_signal(
            barrier, inc=1, device_id=(lax.rem(me + d, ntile), my_lev), device_id_type=MESH
        )
    for d in range(1, nlev):
        pl.semaphore_signal(
            barrier, inc=1, device_id=(me, lax.rem(my_lev + d, nlev)), device_id_type=MESH
        )
    loads = [
        pltpu.make_async_copy(
            ens.at[:, :, pl.ds(c * LANES, LANES)], raw.at[:, :, pl.ds(c * LANES, LANES)], load_sem.at[c]
        )
        for c in range(blocks)
    ]
    list_loads = [
        pltpu.make_async_copy(s, lst.at[i], load_sem.at[blocks])
        for i, s in enumerate((first_in, second_in, bin_in))
    ]
    for c in loads[:1] + list_loads + loads[1:]:
        c.start()

    share = lst.shape[1] // nlev
    quarter = pl.ds(pl.multiple_of(my_lev * share, share), share)

    def list_copy(d):
        peer = (me, lax.rem(my_lev + d, nlev)) if d else (after, my_lev)
        src = plst if d else pack
        return pltpu.make_async_remote_copy(
            src_ref=src.at[:, quarter, :], dst_ref=plst.at[:, quarter, :],
            send_sem=list_sem.at[0], recv_sem=list_sem.at[2 if d else 1],
            device_id=peer, device_id_type=MESH,
        )

    def piece(i, dst, src_rows, src_cols):
        return pltpu.make_async_remote_copy(
            src_ref=own.at[src_rows, src_cols], dst_ref=dst,
            send_sem=halo_send.at[0], recv_sem=halo_recv.at[i],
            device_id=(after, my_lev), device_id_type=MESH,
        )

    near = half // LANES
    halos = [
        piece(c, halo.at[0, pl.ds(0, rows), pl.ds(c * LANES, LANES)], pl.ds(0, rows), pl.ds(c * LANES, LANES))
        for c in range(near)
    ]
    spans = [(a, b, 0, half) for a, b in zip(cuts[:-2], cuts[1:-1])]
    cut = cuts[-2]
    spans += [(cut, rows, 0, half)]
    for i, (a, b, c, n) in enumerate(spans):
        r = pl.ds(a, b - a)
        halos.append(piece(near + i, halo.at[1, r, pl.ds(c, n)], r, pl.ds(half + c, n)))

    loads[0].wait()
    perturb(raw, own, squares, 0)
    pltpu.make_async_copy(lst, lst, load_sem.at[blocks]).wait()
    pack[0] = lst[0] + lst[1] * 65536
    pack[1] = lst[2]
    pl.semaphore_wait(barrier, ntile - 1 + nlev - 1)
    list_copy(0).start()
    halos[0].start()
    for c in range(1, blocks):
        loads[c].wait()
        perturb(raw, own, squares, c * LANES)
        if c < near:
            halos[c].start()
    for d in range(1, nlev):
        pl.semaphore_signal(
            ready, inc=1, device_id=(me, lax.rem(my_lev + d, nlev)), device_id_type=MESH
        )

    def index_rows(ref, i, j):
        return [ref[i, pl.ds(j * groups + g, 1), :] for g in range(groups)]

    def first_rows(j):
        return [r & 65535 for r in index_rows(plst, 0, j)]

    def pairs(j):
        return pl.ds(pl.multiple_of(j * PAIR_CHUNK, PAIR_CHUNK), PAIR_CHUNK)

    def product(a, b):
        return jnp.sum((a * b).reshape(a.shape[0] // lev, lev, PAIR_CHUNK), axis=0)

    def two(x):
        return x[:lev] + x[lev:]

    def corr_parts(cov, ia, ib):
        corr = cov * ia * ib
        hi = corr.astype(jnp.bfloat16).astype(jnp.float32)
        return jnp.concatenate([hi, corr - hi], axis=0).astype(jnp.bfloat16)

    def gather(table, hot):
        return jnp.dot(table, hot, preferred_element_type=jnp.float32)

    def bin_dot(parts, hot):
        return lax.dot_general(
            parts, hot, (((1,), (1,)), ((), ())), preferred_element_type=jnp.float32
        )

    def bin_step(j, carry):
        bin_hot[:, pairs(j)] = onehot(index_rows(lst, 2, j), 0, total_bins)
        return carry

    wide_buf[...] = jnp.zeros_like(wide_buf)
    lax.fori_loop(0, chunks, bin_step, 0)
    ones = jnp.ones((2 * lev, npairs), jnp.bfloat16)
    wide_buf[0, :, pl.ds(0, total_bins)] = bin_dot(ones, bin_hot[...])[:lev]
    counts = wide_buf[0]
    lane = lax.broadcasted_iota(jnp.int32, (lev, LANES), 1)
    level = lax.broadcasted_iota(jnp.int32, (lev, LANES), 0)
    level_squares = jnp.sum(
        jnp.where(lane // BIN_DEV == level + SLOTS // 2, jnp.sum(squares[...], axis=1, keepdims=True), 0.0), axis=0, keepdims=True
    )
    for t in range(ntile):
        early_out[t, 0:1, :] = flatten(counts, t, LANES // 2)
        early_out[t, 1:2, :] = level_squares
    early_in[me] = early_out[me]

    def early_start(d, carry):
        peer = lax.rem(me + d, ntile)
        pltpu.make_async_remote_copy(
            src_ref=early_out.at[peer], dst_ref=early_in.at[me],
            send_sem=early_sem.at[0], recv_sem=early_sem.at[1],
            device_id=(peer, my_lev), device_id_type=MESH,
        ).start()
        return carry

    lax.fori_loop(1, ntile, early_start, 0, unroll=ntile <= 16)

    def wait_all(ref, count, sem):
        part = ref.at[pl.ds(0, count)]
        pltpu.make_async_copy(part, part, sem).wait()


    for c in halos[near:]:
        c.start()

    def own_step(j, carry):
        x = own[...]
        left = gather(x, onehot(index_rows(lst, 0, j), 0, cols))
        right = gather(x, onehot(index_rows(lst, 1, j), 0, cols))
        parts_buf[:, pairs(j)] = corr_parts(
            product(left[:rows], right[:rows]), two(left[rows:]), two(right[rows:]) / (members - 1)
        )
        return carry

    lax.fori_loop(0, chunks // 2, own_step, 0, unroll=OWN)
    list_copy(0).wait_recv()
    for d in range(1, nlev):
        list_copy(d).start()
    lax.fori_loop(chunks // 2, chunks, own_step, 0, unroll=OWN)

    binned = bin_dot(parts_buf[...], bin_hot[...])
    base_buf[...] = two(binned)
    part = plst.at[:, pl.ds(0, (nlev - 1) * share), :]
    pltpu.make_async_copy(part, part, list_sem.at[2]).wait()

    def cross_step(j, carry):
        oh = onehot([(r >> 16) - cols for r in index_rows(plst, 0, j)], 0, cols)
        right = gather(own[...], oh)
        right_buf[j] = right[:rows]
        ib_buf[j] = two(right[rows:]) / (members - 1)
        hot_buf[:, pairs(j)] = onehot(first_rows(j), half, half).astype(HOT)
        pbin_hot[:, pairs(j)] = onehot(index_rows(plst, 1, j), 0, total_bins).astype(HOT)
        return carry

    lax.fori_loop(0, chunks, cross_step, 0, unroll=CROSS)
    pl.semaphore_wait(ready, nlev - 1)

    for c in range(near):
        halos[c].wait_recv()
    halo[0, pl.ds(rows, 2 * lev), :] = inverse_spread(sum_squares(halo.at[0], 0, rows, 0, half, lev), members)

    def near_step(j, carry):
        left = gather(halo[0], onehot(first_rows(j), 0, half))
        cov_buf[j] = product(left[:rows], right_buf[j])
        ia_buf[j] = two(left[rows:])
        return carry

    lax.fori_loop(0, chunks, near_step, 0, unroll=NEAR)
    wait_all(early_in, ntile - 1, early_sem.at[0])
    wait_all(early_in, ntile - 1, early_sem.at[1])
    early = early_in[0]
    for t in range(1, ntile):
        early = early + early_in[t]
    scale[0:1, :] = 1.0 / jnp.maximum(early[0:1], 1.0)
    variance[my_lev] = early[1:2] / ((members - 1) * cols * ntile)
    lev_copies = [
        pltpu.make_async_remote_copy(
            src_ref=variance.at[my_lev], dst_ref=variance.at[my_lev],
            send_sem=early_sem.at[2], recv_sem=early_sem.at[3],
            device_id=(me, lax.rem(my_lev + d, nlev)), device_id_type=MESH,
        )
        for d in range(1, nlev)
    ]
    for c in lev_copies:
        c.start()

    def by_level(row):
        turn = LANES // 2 - BIN_DEV * (lev - 1)
        return pltpu.roll(jnp.broadcast_to(row, (lev, LANES)), turn, 1, stride=BIN_DEV, stride_axis=0)

    far = jnp.zeros((lev, half), jnp.float32)
    kept = rows - cut
    for i, (a, b, c, n) in enumerate(spans):
        halos[near + i].wait_recv()
        sq = sum_squares(halo.at[1], a, b, c, n, lev)
        last = i == len(spans) - 1
        if a < cut:
            far = far + sq
            more = 0
        else:
            halo[1, pl.ds(rows, 2 * lev), pl.ds(c, n)] = inverse_spread(far[:, c:c + n] + sq, members)
            more = 2 * lev

        def far_step(j, acc):
            left = gather(
                halo[1, pl.ds(a, b - a + more), pl.ds(c, n)], hot_buf[pl.ds(c, n), pairs(j)]
            )
            cov = cov_buf[j] + product(left[:b - a], right_buf[j, pl.ds(a, b - a), :])
            ia = ia_buf[j] + two(left[b - a:]) if more else None
            if last:
                parts_buf[:, pairs(j)] = corr_parts(cov, ia, ib_buf[j])
                return acc
            cov_buf[j] = cov
            if more:
                ia_buf[j] = ia
            return acc

        lax.fori_loop(0, chunks, far_step, 0, unroll=True)
        if i == 0:
            wait_all(variance, nlev - 1, early_sem.at[2])
            wait_all(variance, nlev - 1, early_sem.at[3])
        diagonal = lane + level == lev - 1
        packed[lev:lev + 1, :] = jnp.sum(jnp.where(diagonal, by_level(variance[my_lev]), 0.0), axis=0, keepdims=True)
        den = variance[0]
        for v in range(1, nlev):
            den = den + variance[v]
        scale[1:2, :] = 1.0 / jnp.sum(by_level(den), axis=0, keepdims=True)
    wide_buf[1, :, pl.ds(0, total_bins)] = base_buf[...] + two(bin_dot(parts_buf[...], pbin_hot[...]))
    sums = wide_buf[1]
    for t in range(ntile):
        sbuf[t] = flatten(sums, t, LANES // 2)
    mine = my_lev * ntile + me

    def x_start(d, carry):
        dl, dt = d // ntile, d % ntile
        peer_t = lax.rem(me + dt, ntile)
        peer_l = lax.rem(my_lev + dl, nlev)
        pltpu.make_async_remote_copy(
            src_ref=sbuf.at[peer_t], dst_ref=rbuf.at[mine],
            send_sem=x_sem.at[0], recv_sem=x_sem.at[1],
            device_id=(peer_t, peer_l), device_id_type=MESH,
        ).start()
        return carry

    everyone = ntile * nlev
    small = everyone <= 64
    lax.fori_loop(1, everyone, x_start, 0, unroll=small)
    rbuf[mine] = sbuf[me]
    part = own.at[pl.ds(0, rows), :]
    pltpu.make_async_copy(part, part, halo_send.at[0]).wait()
    pltpu.make_async_copy(plst, plst, list_sem.at[0]).wait()
    wait_all(rbuf, everyone - 1, x_sem.at[0])
    wait_all(rbuf, everyone - 1, x_sem.at[1])
    num = jnp.zeros((1, LANES), jnp.float32)
    own_bc = num
    for v in range(nlev):
        tot = rbuf[v * ntile]
        for t in range(1, ntile):
            tot = tot + rbuf[v * ntile + t]
        bc = tot * scale[0:1, :]
        num = num + variance[v] * bc
        own_bc = jnp.where(my_lev == v, bc, own_bc)
    corr = by_level(own_bc)
    for v in range(lev):
        packed[v:v + 1, :] = corr[lev - 1 - v:lev - v]
    packed[lev + 1:lev + 2, :] = jnp.sum(by_level(num), axis=0, keepdims=True) * scale[1:2, :]


def unpack(packed, lv_out, corr_out, avg_out):
    lev = corr_out.shape[0]
    corr_out[...] = packed[0:lev, :BIN_DEV]
    lv_out[...] = packed[lev:lev + 1, :lev]
    avg_out[...] = packed[lev + 1:lev + 2, :BIN_DEV]


def local(ntile, nlev, ensemble, pair_first, pair_second, pair_bin):
    members, lev, cols = ensemble.shape
    npairs = pair_first.shape[0]
    rows = members * lev
    half = cols // 2
    pieces = half // LANES + len(CUTS) + 1
    chunks = npairs // PAIR_CHUNK
    total_bins = BIN_DEV * ntile
    bin_lanes = -(-total_bins // LANES) * LANES
    f32, bf16 = jnp.float32, jnp.bfloat16
    idx = [x.reshape(npairs // LANES, LANES) for x in (pair_first, pair_second, pair_bin)]
    vmem = pl.BlockSpec(memory_space=pltpu.VMEM)
    hbm = pl.BlockSpec(memory_space=pl.ANY)
    packed = pl.pallas_call(
        functools.partial(kernel, ntile, nlev),
        out_shape=jax.ShapeDtypeStruct((2 * lev, LANES), f32),
        in_specs=[hbm] * 4,
        out_specs=vmem,
        scratch_shapes=[
            pltpu.VMEM((members, lev, cols), bf16),
            pltpu.VMEM((rows + 2 * lev, cols), bf16),
            pltpu.VMEM((2, rows + 2 * lev, half), bf16),
            pltpu.VMEM((3, npairs // LANES, LANES), jnp.int32),
            *[pltpu.VMEM((2, npairs // LANES, LANES), jnp.int32)] * 2,
            pltpu.VMEM((lev, cols), f32),
            pltpu.VMEM((chunks, rows, PAIR_CHUNK), f32),
            *[pltpu.VMEM((chunks, lev, PAIR_CHUNK), f32)] * 3,
            pltpu.VMEM((half, npairs), HOT),
            pltpu.VMEM((total_bins, npairs), bf16),
            pltpu.VMEM((total_bins, npairs), HOT),
            pltpu.VMEM((2 * lev, npairs), bf16),
            pltpu.VMEM((lev, total_bins), f32),
            pltpu.VMEM((2, lev, bin_lanes), f32),
            *[pltpu.VMEM((ntile, 2, LANES), f32)] * 2,
            pltpu.VMEM((nlev, 1, LANES), f32),
            pltpu.VMEM((2, LANES), f32),
            pltpu.VMEM((ntile, 1, LANES), f32),
            pltpu.VMEM((nlev * ntile, 1, LANES), f32),
            pltpu.SemaphoreType.DMA((cols // LANES + 1,)),
            pltpu.SemaphoreType.DMA((1,)),
            pltpu.SemaphoreType.DMA((pieces,)),
            pltpu.SemaphoreType.DMA((3,)),
            pltpu.SemaphoreType.DMA((4,)),
            pltpu.SemaphoreType.DMA((2,)),
            pltpu.SemaphoreType.REGULAR,
        ],
        compiler_params=pltpu.CompilerParams(
            collective_id=0, has_side_effects=True, vmem_limit_bytes=55220 * 1024
        ),
        name="binned_corr",
    )(ensemble, *idx)
    lv, corr, avg = pl.pallas_call(
        unpack,
        out_shape=(
            jax.ShapeDtypeStruct((1, lev), f32),
            jax.ShapeDtypeStruct((lev, BIN_DEV), f32),
            jax.ShapeDtypeStruct((1, BIN_DEV), f32),
        ),
        in_specs=[vmem],
        out_specs=(vmem, vmem, vmem),
        compiler_params=pltpu.CompilerParams(vmem_limit_bytes=4 * 1024 * 1024),
        name="unpack",
    )(packed)
    return lv.reshape(lev), corr, avg.reshape(BIN_DEV)


def solution(mesh):
    in_specs = (P(None, "lev", "tile"), P("tile"), P("tile"), P("tile"))
    out_specs = (P("lev"), P("lev", "tile"), P("tile"))
    body = functools.partial(local, mesh.shape["tile"], mesh.shape["lev"])
    return jax.shard_map(body, mesh=mesh, in_specs=in_specs, out_specs=out_specs, check_vma=False)
```
